32 devices in a mesh: row: 4 (over x, core), col: 8 (over z, y).
Axes of the slice: x: 2, y: 2, z: 4, core: 2. Of those that a mesh axis runs over, the one named last changes fastest.
Arguments:
- tokens: bfloat16 [16384, 1024], P(('row', 'col')), may hold values from -6 to 6
- expert_ids: int32 [16384, 1], P(('row', 'col')), may hold values from 0 to 31; in each aligned block of 512 rows (0 to 511, 512 to 1023, ...) at most 32 rows name the same one
- gate_prob: float32 [16384], P(('row', 'col')), may hold values from 0.25 to 1
- norm_gain: float32 [1024], replicated, may hold values from 0.1 to 1.9
- weight_in: bfloat16 [32, 1024, 4096], P(('row', 'col')), may hold values from -0.1875 to 0.1875
- weight_out: bfloat16 [32, 4096, 1024], P(('row', 'col')), may hold values from -0.09375 to 0.09375
Outputs:
- mixed: bfloat16 [16384, 1024], P(('row', 'col'))
- routed: int32 [32], P(('row', 'col'))
The draws below stay inside these ranges and needn't reach their ends.
Inputs may be any that keep to these rules, and one draw needn't show every extreme that they name: `expert_ids`: among the 512 tokens of one device no expert is chosen more than 32 times; some expert is chosen exactly 32 times by some device's tokens.
All inputs are finite; a program needn't handle non-finite values.
Results may differ from the reference program's by a relative error of at most 0.001.
The reference program's roundings to bfloat16 on the way (of `normed`, `slots`, `hidden` and `answers`) count: a program that leaves them out, or rounds other values in their place, can miss the bound.
Values may be sent and summed in bfloat16 or wider, within the bound.
A program may use at most 64 MiB of HBM per device.

```python
import math
import jax
import jax.numpy as jnp
import numpy as np
from jax import lax

D = 1024
FF = 4096
TOK_DEV = 512
EXPERTS = 32
CAP = 32
TOKENS = 16384
DEVICES = 32


def draw_tokens(key, part):
    base_key = jax.random.fold_in(key, 11)
    value_key, sparse_key, choose_key = jax.random.split(base_key, 3)
    values = jnp.clip(jax.random.normal(value_key, (TOKENS, D), jnp.float32), -6.0, 6.0)
    sparse_rows = jax.random.randint(sparse_key, (TOKENS,), 0, 64) == 0
    chosen = jax.random.randint(choose_key, (TOKENS // TOK_DEV,), 0, TOK_DEV)
    position = jnp.arange(TOKENS, dtype=jnp.int32)
    block_index = position // TOK_DEV
    forced_rows = position % TOK_DEV == chosen[block_index]
    kept_rows = jnp.logical_not(jnp.logical_or(sparse_rows, forced_rows)).astype(jnp.float32)
    return (values * kept_rows[:, None]).astype(jnp.bfloat16)


def levels(key, dims, cuts, low, high):
    level, own = 1.0, jax.random.fold_in(key, 6)
    for dim, parts in cuts:
        steps = jnp.exp(jax.random.uniform(jax.random.fold_in(own, dim), (parts,), jnp.float32, low / len(cuts), high / len(cuts)))
        level = level * jnp.repeat(steps, dims[dim] // parts).reshape([-1 if axis == dim else 1 for axis in range(len(dims))])
    return level


def routed_block(own_key, own, number, rows, number_of, top, reach, lean):
    order = jax.random.permutation(own_key, number_of)
    heavy_load, usual = portions_of(number_of, rows * top, reach, lean, True), portions_of(number_of, rows * top, reach, lean, False)
    places = jnp.arange(number_of)

    def named(tallies, offset_by):
        used = int((tallies > 0).sum())
        fixed = max(1, used // 4)
        moved = fixed + (places - fixed + offset_by * (used - fixed)) % max(1, number_of - fixed)
        return jnp.zeros((number_of,), jnp.int32).at[order[jnp.where(places < fixed, places, moved)]].set(jnp.asarray(tallies, jnp.int32))

    tallies = jnp.where(number % 4 == 0, named(heavy_load, number // 4), named(usual, number - number // 4 - 1))
    mixed = jax.random.permutation(jax.random.fold_in(own, 3), number_of)
    donor, sink = mixed[0:number_of // 2 * 2:2], mixed[1:number_of // 2 * 2:2]
    room = jnp.minimum(tallies[donor] - 1, reach - tallies[sink]) // 2
    room = jnp.where((donor == order[0]) | (sink == order[0]) | (tallies[sink] == 0), 0, jnp.maximum(room, 0))
    moved = jax.random.randint(jax.random.fold_in(own, 4), (number_of // 2,), 0, 1 << 20) % (room + 1)
    tallies = tallies.at[donor].add(-moved).at[sink].add(moved)
    labels = jnp.searchsorted(jnp.cumsum(tallies), jnp.arange(rows * top), side="right").astype(jnp.int32)
    table = labels.reshape(top, rows).T
    table = table[jax.random.permutation(jax.random.fold_in(own, 1), rows)]
    offset_by = jax.random.randint(jax.random.fold_in(own, 2), (rows, 1), 0, top)
    return jnp.take_along_axis(table, (jnp.arange(top)[None, :] + offset_by) % top, axis=1)


def portions_of(number_of, total, reach, skew, full):
    weights = [(1 << 20) // math.isqrt(rank ** skew) + 1 for rank in range(1, number_of + 1)]
    largest = reach if full else min(reach, max(-(-total // number_of), total * weights[0] // sum(weights)))
    least = 1 if total - largest >= number_of - 1 else 0
    holding, rest = [largest] + [least] * (number_of - 1), total - largest - least * (number_of - 1)
    while rest > 0:
        candidates = [i for i in range(1, number_of) if holding[i] < largest] or [i for i in range(1, number_of) if holding[i] < reach]
        pool, budget = sum([weights[i] for i in candidates]), rest
        for i in candidates:
            more = min(reach - holding[i], max(1, budget * weights[i] // pool), rest)
            holding[i] = holding[i] + more
            rest = rest - more
    return np.array(holding)


def normal_values(stream_key, dims, width, reach, shards=(), held_as=jnp.bfloat16):
    entries = jax.random.normal(stream_key, dims, jnp.float32) * width
    if len(shards) > 0:
        entries = levels(stream_key, dims, shards, -0.22, 0.18) * entries
    return jnp.clip(entries, min=-reach, max=reach).astype(held_as)


def setup_inputs(seed: int = 0) -> dict:
    seeds = jax.random.split(jax.random.key(seed), 7)
    tokens = draw_tokens(jax.random.fold_in(seeds[6], 71), 0)
    expert_ids_keys = jax.random.split(jax.random.fold_in(seeds[1], 1), TOKENS // TOK_DEV)
    expert_ids_turns = jax.random.permutation(jax.random.fold_in(seeds[1], 3), TOKENS // TOK_DEV)
    expert_ids = jax.vmap(lambda own, number: routed_block(jax.random.fold_in(seeds[1], 2), own, number, TOK_DEV, EXPERTS, 1, CAP, 2))(expert_ids_keys, expert_ids_turns).reshape((TOKENS, 1))
    gate_prob = jnp.clip(0.25 + 0.75 * jax.random.uniform(seeds[2], (TOKENS,), jnp.float32) ** levels(seeds[2], (TOKENS,), ((0, 32),), -0.2, 0.2), 0.25, 1.0)
    norm_gain = jnp.clip(1.0 + 0.18 * jax.random.normal(seeds[3], (D,), jnp.float32), 0.1, 1.9)
    weight_in = normal_values(seeds[4], (EXPERTS, D, FF), D ** -0.5, 0.1875, ((0, 32),))
    weight_out = normal_values(seeds[5], (EXPERTS, FF, D), FF ** -0.5, 0.09375, ((0, 32),))
    return {"tokens": tokens, "expert_ids": expert_ids, "gate_prob": gate_prob, "norm_gain": norm_gain, "weight_in": weight_in, "weight_out": weight_out}


def slot_rank(block_ids):
    count = block_ids.shape[0]
    same = block_ids[:, None] == block_ids[None, :]
    earlier = jnp.arange(count, dtype=jnp.int32)[None, :] < jnp.arange(count, dtype=jnp.int32)[:, None]
    return lax.optimization_barrier(jnp.sum((same & earlier).astype(jnp.int32), axis=1)).astype(jnp.int32)

def expert_ffn(pieces):
    slab, first, second = pieces
    hidden = jnp.maximum(jnp.dot(slab, first, preferred_element_type=jnp.float32), 0.0).astype(jnp.bfloat16)
    return jnp.dot(hidden, second, preferred_element_type=jnp.float32).astype(jnp.bfloat16)

def reference(tokens, expert_ids, gate_prob, norm_gain, weight_in, weight_out):
    flat_ids = expert_ids[:, 0].astype(jnp.int32)
    within = jax.vmap(slot_rank)(flat_ids.reshape(DEVICES, TOK_DEV)).reshape(-1)
    source = (jnp.arange(TOKENS, dtype=jnp.int32) // TOK_DEV).astype(jnp.int32)
    placed = ((flat_ids * DEVICES + source) * CAP + within).astype(jnp.int32)
    wide = tokens.astype(jnp.float32)
    scale = lax.rsqrt(lax.optimization_barrier(jnp.mean(wide * wide, axis=1, keepdims=True)) + 1e-06)
    normed = (wide * scale * norm_gain[None, :]).astype(jnp.bfloat16)
    slots = jnp.zeros((EXPERTS * DEVICES * CAP, D), jnp.bfloat16).at[placed].set(normed)
    slots = slots.reshape(EXPERTS, DEVICES * CAP, D)
    answers = lax.map(expert_ffn, (slots, weight_in, weight_out))
    back = answers.reshape(EXPERTS * DEVICES * CAP, D)[placed]
    mixed = (wide + gate_prob[:, None] * back.astype(jnp.float32)).astype(jnp.bfloat16)
    routed = lax.optimization_barrier(jnp.sum((flat_ids[:, None] == jnp.arange(EXPERTS, dtype=jnp.int32)[None, :]).astype(jnp.int32), axis=0))
    return (mixed, routed)
```

```python
import functools

import jax
import jax.numpy as jnp
from jax import lax
from jax.experimental import pallas as pl
from jax.experimental.pallas import tpu as pltpu
from jax.sharding import PartitionSpec as P

MESH = pl.DeviceIdType.MESH


def bit_xor(a, b, size):
    out, unit = 0, 1
    while unit < size:
        out = out + lax.rem(lax.div(a, unit) + lax.div(b, unit), 2) * unit
        unit *= 2
    return out


def kernel(
    rows, cols, cap, groups, ff_tile, out_tile,
    tokens_ref, ids_col_ref, ids_row_ref, gain_ref, first_hbm, second_hbm,
    back_ref, routed_ref,
    first, second, normed, outgoing, received, answers, returned, hidden, total,
    counts, counts_in, placed_col,
    weight_sem, send_sem, recv_sem, ret_sem, count_sem,
):
    n = rows * cols
    tok_rows, width = tokens_ref.shape
    lanes = counts.shape[1]
    per = n // groups
    span = per * cap
    my_row, my_col = lax.axis_index("row"), lax.axis_index("col")
    me = my_row * cols + my_col

    def partner(place):
        q = n - 1 - place
        return (
            bit_xor(my_row, lax.rem(q, rows), rows),
            bit_xor(my_col, lax.div(q, rows), cols),
        )

    barrier = pltpu.get_barrier_semaphore()

    @pl.loop(0, n - 1)
    def _(place):
        pl.semaphore_signal(barrier, inc=1, device_id=partner(place), device_id_type=MESH)

    load_first = pltpu.make_async_copy(first_hbm.at[0], first, weight_sem.at[0])
    load_second = pltpu.make_async_copy(second_hbm.at[0], second, weight_sem.at[1])
    load_first.start()
    load_second.start()

    def slot_of(ids, within):
        offset = jnp.bitwise_xor(ids, me)
        q = (offset % cols) * rows + offset // cols
        return (n - 1 - q) * cap + within

    ids_row = ids_row_ref[...]
    ids_col = ids_col_ref[...]
    at_row = lax.broadcasted_iota(jnp.int32, (tok_rows, tok_rows), 0)
    at_col = lax.broadcasted_iota(jnp.int32, (tok_rows, tok_rows), 1)
    hot_row = lax.broadcasted_iota(jnp.int32, (lanes, tok_rows), 0) == ids_row
    before = jnp.where(at_row < at_col, 1.0, 0.0).astype(jnp.bfloat16)
    earlier = jnp.dot(
        jnp.where(hot_row, 1.0, 0.0).astype(jnp.bfloat16), before, preferred_element_type=jnp.float32
    )
    within_row = jnp.sum(jnp.where(hot_row, earlier, 0.0), axis=0, keepdims=True)
    placed_row = slot_of(ids_row, within_row.astype(jnp.int32))

    wide = tokens_ref[...].astype(jnp.float32)
    scale = lax.rsqrt(jnp.mean(wide * wide, axis=1, keepdims=True) + 1e-06)
    normed[...] = (wide * scale * gain_ref[...]).astype(jnp.bfloat16)

    def as_blocks(values):
        return values.reshape(per, cap, width).astype(jnp.bfloat16)

    def as_rows(ref, g):
        blocks = ref[pl.ds(g * per, per)]
        if cap % 16 == 0:
            return blocks.reshape(span, width)
        return blocks.astype(jnp.float32).reshape(span, width).astype(jnp.bfloat16)

    def exchange(source, target, sem, out_sem, g):
        @pl.loop(0, per)
        def _(i):
            place = g * per + i

            @pl.when(place < n - 1)
            def _():
                pltpu.make_async_remote_copy(
                    src_ref=source.at[place],
                    dst_ref=target.at[place],
                    send_sem=out_sem,
                    recv_sem=sem.at[g],
                    device_id=partner(place),
                    device_id_type=MESH,
                ).start()

            @pl.when(place == n - 1)
            def _():
                pltpu.make_async_copy(source.at[n - 1], target.at[n - 1], sem.at[g]).start()

    def wait_group(target, sem, g):
        whole = target.at[pl.ds(g * per, per)]
        pltpu.make_async_copy(whole, whole, sem.at[g]).wait()

    @pl.loop(0, groups)
    def _(g):
        slot = lax.broadcasted_iota(jnp.int32, (span, tok_rows), 0) + g * span
        table = jnp.where(slot == placed_row, 1.0, 0.0).astype(jnp.bfloat16)
        outgoing[pl.ds(g * per, per)] = as_blocks(
            jnp.dot(table, normed[...], preferred_element_type=jnp.float32)
        )

        @pl.when(g == 0)
        def _():
            pl.semaphore_wait(barrier, n - 1)

        exchange(outgoing, received, recv_sem, send_sem.at[0], g)

    hot_col = lax.broadcasted_iota(jnp.int32, (tok_rows, lanes), 1) == ids_col
    ones_col = jnp.where(hot_col, 1.0, 0.0)
    counts[...] = jnp.sum(ones_col, axis=0, keepdims=True)
    after = jnp.where(at_col < at_row, 1.0, 0.0).astype(jnp.bfloat16)
    earlier_col = jnp.dot(after, ones_col.astype(jnp.bfloat16), preferred_element_type=jnp.float32)
    within_col = jnp.sum(jnp.where(hot_col, earlier_col, 0.0), axis=1, keepdims=True)
    placed_col[...] = slot_of(ids_col, within_col.astype(jnp.int32))
    total[...] = jnp.zeros_like(total)

    @pl.loop(0, n - 1)
    def _(place):
        pltpu.make_async_remote_copy(
            src_ref=counts,
            dst_ref=counts_in.at[place],
            send_sem=send_sem.at[2],
            recv_sem=count_sem,
            device_id=partner(place),
            device_id_type=MESH,
        ).start()

    load_first.wait()
    load_second.wait()

    @pl.loop(0, groups)
    def _(step):
        g = lax.rem(step + groups - 1, groups)
        wait_group(received, recv_sem, g)
        slab = as_rows(received, g)

        @pl.loop(0, first.shape[1] // ff_tile)
        def _(i):
            part = pl.ds(pl.multiple_of(i * ff_tile, ff_tile), ff_tile)
            grown = jnp.dot(slab, first[:, part], preferred_element_type=jnp.float32)
            hidden[:, part] = jnp.maximum(grown, 0.0).astype(jnp.bfloat16)

        @pl.loop(0, width // out_tile)
        def _(i):
            part = pl.ds(pl.multiple_of(i * out_tile, out_tile), out_tile)
            made = jnp.dot(hidden[...], second[:, part], preferred_element_type=jnp.float32)
            answers[pl.ds(g * per, per), :, part] = made.reshape(per, cap, out_tile).astype(
                jnp.bfloat16
            )

        exchange(answers, returned, ret_sem, send_sem.at[1], g)

    arrived = counts_in.at[pl.ds(0, n - 1)]
    pltpu.make_async_copy(arrived, arrived, count_sem).wait()
    sums = jnp.sum(counts_in[pl.ds(0, n - 1)], axis=0) + counts[...]
    mine = lax.broadcasted_iota(jnp.int32, (1, lanes), 1) == me
    routed_ref[0] = jnp.sum(jnp.where(mine, sums, 0.0)).astype(jnp.int32)

    @pl.loop(0, groups)
    def _(step):
        g = lax.rem(step + groups - 1, groups)
        wait_group(returned, ret_sem, g)
        slot = lax.broadcasted_iota(jnp.int32, (tok_rows, span), 1) + g * span
        table = jnp.where(slot == placed_col[...], 1.0, 0.0).astype(jnp.bfloat16)
        total[...] += jnp.dot(table, as_rows(returned, g), preferred_element_type=jnp.float32)

    back_ref[...] = total[...].astype(jnp.bfloat16)

    sent = outgoing.at[pl.ds(0, n - 1)]
    pltpu.make_async_copy(sent, sent, send_sem.at[0]).wait()
    pltpu.make_async_copy(sent, sent, send_sem.at[1]).wait()
    pltpu.make_async_copy(arrived, arrived, send_sem.at[2]).wait()


def on_device(rows, cols, tokens, expert_ids, gate_prob, norm_gain, weight_in, weight_out):
    tok_rows, width = tokens.shape
    hidden_width = weight_in.shape[2]
    n = rows * cols
    cap = 2 * tok_rows // n
    lanes = -(-n // 128) * 128
    per = max(1, min(n, 256 // cap))
    groups = n // per
    vmem = pl.BlockSpec(memory_space=pltpu.VMEM)
    hbm = pl.BlockSpec(memory_space=pl.ANY)
    block = pltpu.VMEM((n, cap, width), jnp.bfloat16)
    back, routed = pl.pallas_call(
        functools.partial(kernel, rows, cols, cap, groups, min(512, hidden_width), min(256, width)),
        out_shape=(
            jax.ShapeDtypeStruct((tok_rows, width), jnp.bfloat16),
            jax.ShapeDtypeStruct((1,), jnp.int32),
        ),
        in_specs=[vmem, vmem, vmem, vmem, hbm, hbm],
        out_specs=(vmem, pl.BlockSpec(memory_space=pltpu.SMEM)),
        scratch_shapes=[
            pltpu.VMEM((width, hidden_width), jnp.bfloat16),
            pltpu.VMEM((hidden_width, width), jnp.bfloat16),
            pltpu.VMEM((tok_rows, width), jnp.bfloat16),
            block, block, block, block,
            pltpu.VMEM((per * cap, hidden_width), jnp.bfloat16),
            pltpu.VMEM((tok_rows, width), jnp.float32),
            pltpu.VMEM((1, lanes), jnp.float32),
            pltpu.VMEM((n, 1, lanes), jnp.float32),
            pltpu.VMEM((tok_rows, 1), jnp.int32),
            pltpu.SemaphoreType.DMA((2,)),
            pltpu.SemaphoreType.DMA((3,)),
            pltpu.SemaphoreType.DMA((groups,)),
            pltpu.SemaphoreType.DMA((groups,)),
            pltpu.SemaphoreType.DMA,
        ],
        compiler_params=pltpu.CompilerParams(
            collective_id=0, has_side_effects=True, vmem_limit_bytes=56 * 1024 * 1024
        ),
    )(
        tokens,
        expert_ids,
        expert_ids.reshape(1, tok_rows),
        norm_gain.reshape(1, width),
        weight_in,
        weight_out,
    )
    wide = tokens.astype(jnp.float32)
    mixed = (wide + gate_prob[:, None] * back.astype(jnp.float32)).astype(jnp.bfloat16)
    return (mixed, routed)


def solution(mesh):
    return jax.shard_map(
        functools.partial(on_device, mesh.shape["row"], mesh.shape["col"]),
        mesh=mesh,
        in_specs=(
            P(("row", "col"), None),
            P(("row", "col"), None),
            P(("row", "col")),
            P(),
            P(("row", "col"), None, None),
            P(("row", "col"), None, None),
        ),
        out_specs=(P(("row", "col"), None), P(("row", "col"))),
        check_vma=False,
    )
```

```python
import functools

import jax
import jax.numpy as jnp
from jax import lax
from jax.experimental import pallas as pl
from jax.experimental.pallas import tpu as pltpu
from jax.sharding import PartitionSpec as P

MESH = pl.DeviceIdType.MESH


def bit_xor(a, b, size):
    out, unit = 0, 1
    while unit < size:
        out = out + lax.rem(lax.div(a, unit) + lax.div(b, unit), 2) * unit
        unit *= 2
    return out


def kernel(
    rows, cols, cap, groups, ff_tile, out_tile,
    tokens_ref, ids_row_ref, gain_ref, first_hbm, second_hbm,
    back_ref, routed_ref,
    first, second, normed, outgoing, received, answers, returned, hidden, total,
    counts, counts_in, placed_col,
    weight_sem, send_sem, recv_sem, ret_sem, count_sem,
):
    n = rows * cols
    tok_rows, width = tokens_ref.shape
    lanes = counts.shape[1]
    per = n // groups
    span = per * cap
    my_row, my_col = lax.axis_index("row"), lax.axis_index("col")
    me = my_row * cols + my_col

    def turn(step):
        if groups % 2:
            return step
        return lax.rem(step, 2) * (groups // 2) + lax.div(step, 2)

    def partner(place):
        q = n - 1 - place
        return (
            bit_xor(my_row, lax.rem(q, rows), rows),
            bit_xor(my_col, lax.div(q, rows), cols),
        )

    barrier = pltpu.get_barrier_semaphore()

    @pl.loop(0, n - 1)
    def _(place):
        pl.semaphore_signal(barrier, inc=1, device_id=partner(place), device_id_type=MESH)

    load_first = pltpu.make_async_copy(first_hbm.at[0], first, weight_sem.at[0])
    load_second = pltpu.make_async_copy(second_hbm.at[0], second, weight_sem.at[1])
    load_first.start()
    load_second.start()

    def slot_of(ids, within):
        offset = jnp.bitwise_xor(ids, me)
        q = (offset % cols) * rows + offset // cols
        return (n - 1 - q) * cap + within

    ids_row = ids_row_ref[...]
    at_row = lax.broadcasted_iota(jnp.int32, (tok_rows, tok_rows), 0)
    at_col = lax.broadcasted_iota(jnp.int32, (tok_rows, tok_rows), 1)
    hot_row = lax.broadcasted_iota(jnp.int32, (lanes, tok_rows), 0) == ids_row
    before = jnp.where(at_row < at_col, 1.0, 0.0).astype(jnp.bfloat16)
    earlier = jnp.dot(
        jnp.where(hot_row, 1.0, 0.0).astype(jnp.bfloat16), before, preferred_element_type=jnp.float32
    )
    within_row = jnp.sum(jnp.where(hot_row, earlier, 0.0), axis=0, keepdims=True)
    placed_row = slot_of(ids_row, within_row.astype(jnp.int32))

    wide = tokens_ref[...].astype(jnp.float32)
    scale = lax.rsqrt(jnp.mean(wide * wide, axis=1, keepdims=True) + 1e-06)
    normed[...] = (wide * scale * gain_ref[...]).astype(jnp.bfloat16)

    def as_blocks(values):
        return values.reshape(per, cap, width).astype(jnp.bfloat16)

    def as_rows(ref, g):
        blocks = ref[pl.ds(g * per, per)]
        if cap % 16 == 0:
            return blocks.reshape(span, width)
        return blocks.astype(jnp.float32).reshape(span, width).astype(jnp.bfloat16)

    def exchange(source, target, sem, out_sem, g):
        @pl.loop(0, per)
        def _(i):
            place = g * per + i

            @pl.when(place < n - 1)
            def _():
                pltpu.make_async_remote_copy(
                    src_ref=source.at[place],
                    dst_ref=target.at[place],
                    send_sem=out_sem,
                    recv_sem=sem.at[g],
                    device_id=partner(place),
                    device_id_type=MESH,
                ).start()

            @pl.when(place == n - 1)
            def _():
                pltpu.make_async_copy(source.at[n - 1], target.at[n - 1], sem.at[g]).start()

    def wait_group(target, sem, g):
        whole = target.at[pl.ds(g * per, per)]
        pltpu.make_async_copy(whole, whole, sem.at[g]).wait()

    @pl.loop(0, groups)
    def _(step):
        g = turn(step)
        slot = lax.broadcasted_iota(jnp.int32, (span, tok_rows), 0) + g * span
        table = jnp.where(slot == placed_row, 1.0, 0.0).astype(jnp.bfloat16)
        outgoing[pl.ds(g * per, per)] = as_blocks(
            jnp.dot(table, normed[...], preferred_element_type=jnp.float32)
        )

        @pl.when(step == 0)
        def _():
            pl.semaphore_wait(barrier, n - 1)

        exchange(outgoing, received, recv_sem, send_sem.at[0], g)

    counts[...] = lax.dot_general(
        jnp.ones((8, tok_rows), jnp.bfloat16),
        jnp.where(hot_row, 1.0, 0.0).astype(jnp.bfloat16),
        (((1,), (1,)), ((), ())),
        preferred_element_type=jnp.float32,
    )[0:1]
    turned = jnp.where(at_row == at_col, placed_row.astype(jnp.float32), 0.0)
    placed_col[...] = jnp.sum(turned, axis=1, keepdims=True).astype(jnp.int32)
    total[...] = jnp.zeros_like(total)

    @pl.loop(0, n - 1)
    def _(place):
        pltpu.make_async_remote_copy(
            src_ref=counts,
            dst_ref=counts_in.at[place],
            send_sem=send_sem.at[2],
            recv_sem=count_sem,
            device_id=partner(place),
            device_id_type=MESH,
        ).start()

    load_first.wait()
    load_second.wait()

    @pl.loop(0, groups)
    def _(step):
        g = turn(lax.rem(step + groups - 1, groups))
        wait_group(received, recv_sem, g)
        slab = as_rows(received, g)

        @pl.loop(0, first.shape[1] // ff_tile)
        def _(i):
            part = pl.ds(pl.multiple_of(i * ff_tile, ff_tile), ff_tile)
            grown = jnp.dot(slab, first[:, part], preferred_element_type=jnp.float32)
            hidden[:, part] = jnp.maximum(grown, 0.0).astype(jnp.bfloat16)

        @pl.loop(0, width // out_tile)
        def _(i):
            part = pl.ds(pl.multiple_of(i * out_tile, out_tile), out_tile)
            made = jnp.dot(hidden[...], second[:, part], preferred_element_type=jnp.float32)
            answers[pl.ds(g * per, per), :, part] = made.reshape(per, cap, out_tile).astype(
                jnp.bfloat16
            )

        exchange(answers, returned, ret_sem, send_sem.at[1], g)

    arrived = counts_in.at[pl.ds(0, n - 1)]
    pltpu.make_async_copy(arrived, arrived, count_sem).wait()
    sums = jnp.sum(counts_in[pl.ds(0, n - 1)], axis=0) + counts[...]
    mine = lax.broadcasted_iota(jnp.int32, (1, lanes), 1) == me
    routed_ref[0] = jnp.sum(jnp.where(mine, sums, 0.0)).astype(jnp.int32)

    @pl.loop(0, groups)
    def _(step):
        g = turn(lax.rem(step + groups - 1, groups))
        wait_group(returned, ret_sem, g)
        slot = lax.broadcasted_iota(jnp.int32, (tok_rows, span), 1) + g * span
        table = jnp.where(slot == placed_col[...], 1.0, 0.0).astype(jnp.bfloat16)
        total[...] += jnp.dot(table, as_rows(returned, g), preferred_element_type=jnp.float32)

    back_ref[...] = total[...].astype(jnp.bfloat16)

    sent = outgoing.at[pl.ds(0, n - 1)]
    pltpu.make_async_copy(sent, sent, send_sem.at[0]).wait()
    pltpu.make_async_copy(sent, sent, send_sem.at[1]).wait()
    pltpu.make_async_copy(arrived, arrived, send_sem.at[2]).wait()


def on_device(rows, cols, tokens, expert_ids, gate_prob, norm_gain, weight_in, weight_out):
    tok_rows, width = tokens.shape
    hidden_width = weight_in.shape[2]
    n = rows * cols
    cap = 2 * tok_rows // n
    lanes = -(-n // 128) * 128
    per = max(1, min(n, 256 // cap))
    groups = n // per
    vmem = pl.BlockSpec(memory_space=pltpu.VMEM)
    hbm = pl.BlockSpec(memory_space=pl.ANY)
    block = pltpu.VMEM((n, cap, width), jnp.bfloat16)
    back, routed = pl.pallas_call(
        functools.partial(kernel, rows, cols, cap, groups, min(512, hidden_width), min(256, width)),
        out_shape=(
            jax.ShapeDtypeStruct((tok_rows, width), jnp.bfloat16),
            jax.ShapeDtypeStruct((1,), jnp.int32),
        ),
        in_specs=[vmem, vmem, vmem, hbm, hbm],
        out_specs=(vmem, pl.BlockSpec(memory_space=pltpu.SMEM)),
        scratch_shapes=[
            pltpu.VMEM((width, hidden_width), jnp.bfloat16),
            pltpu.VMEM((hidden_width, width), jnp.bfloat16),
            pltpu.VMEM((tok_rows, width), jnp.bfloat16),
            block, block, block, block,
            pltpu.VMEM((per * cap, hidden_width), jnp.bfloat16),
            pltpu.VMEM((tok_rows, width), jnp.float32),
            pltpu.VMEM((1, lanes), jnp.float32),
            pltpu.VMEM((n, 1, lanes), jnp.float32),
            pltpu.VMEM((tok_rows, 1), jnp.int32),
            pltpu.SemaphoreType.DMA((2,)),
            pltpu.SemaphoreType.DMA((3,)),
            pltpu.SemaphoreType.DMA((groups,)),
            pltpu.SemaphoreType.DMA((groups,)),
            pltpu.SemaphoreType.DMA,
        ],
        compiler_params=pltpu.CompilerParams(
            collective_id=0, has_side_effects=True, vmem_limit_bytes=56 * 1024 * 1024
        ),
    )(
        tokens,
        expert_ids.reshape(1, tok_rows),
        norm_gain.reshape(1, width),
        weight_in,
        weight_out,
    )
    wide = tokens.astype(jnp.float32)
    mixed = (wide + gate_prob[:, None] * back.astype(jnp.float32)).astype(jnp.bfloat16)
    return (mixed, routed)


def solution(mesh):
    return jax.shard_map(
        functools.partial(on_device, mesh.shape["row"], mesh.shape["col"]),
        mesh=mesh,
        in_specs=(
            P(("row", "col"), None),
            P(("row", "col"), None),
            P(("row", "col")),
            P(),
            P(("row", "col"), None, None),
            P(("row", "col"), None, None),
        ),
        out_specs=(P(("row", "col"), None), P(("row", "col"))),
        check_vma=False,
    )
```
